32 devices in a mesh: row: 8 (over z, y), col: 4 (over x, core).
Axes of the slice: x: 2, y: 2, z: 4, core: 2. Of those that a mesh axis runs over, the one named last changes fastest.
Arguments:
- eigvecs: float32 [131072, 1024], P('row', 'col'), may hold values from -6 to 6
- reflectors: float32 [4, 131072, 256], P(None, ('row', 'col'))
- factors: float32 [4, 256, 256], replicated, as said below
Outputs:
- transformed: float32 [131072, 1024], P('row', 'col')
The draws below stay inside these ranges and needn't reach their ends.
Inputs may be any that keep to these rules, and one draw needn't show every extreme that they name: Each factors[k] is upper triangular with a positive diagonal.
All inputs are finite; a program needn't handle non-finite values.
Results may differ from the reference program's by a relative error of at most 0.00012.
Values sent between devices are 32-bit elements; how exact they have to be, the bound alone decides.
A program may use at most 192 MiB of HBM per device.

```python
import jax
import jax.numpy as jnp
from jax import lax

N = 131072
M = 1024
WB = 256
PANELS = 4


def draw_reflectors(key, part):
    scale = (N * WB) ** (-0.25)
    base = jnp.clip(jax.random.normal(key, (PANELS, N, WB), jnp.float32), -6.0, 6.0)
    return base * scale


def draw_factors(key, part):
    diag = jax.random.uniform(key, (PANELS, WB), jnp.float32, 0.5, 1.5)
    off = 0.5 * jnp.clip(jax.random.normal(jax.random.fold_in(key, 3), (PANELS, WB, WB), jnp.float32), -6.0, 6.0) / jnp.sqrt(WB * 1.0)
    upper = jnp.triu(off, 1)
    eye = jnp.eye(WB, dtype=jnp.float32)
    return upper + eye[None, :, :] * diag[:, None, :]


def block_scale(rng, dims, pieces, low, top_value):
    def one(position, parts):
        heights = jax.random.uniform(jax.random.fold_in(jax.random.fold_in(rng, 6), position), (parts,), jnp.float32, low / len(pieces), top_value / len(pieces))
        return jnp.repeat(jnp.exp(heights), dims[position] // parts).reshape((-1,) + (1,) * (len(dims) - position - 1))

    factor_of = one(*pieces[0])
    for cut in pieces[1:]:
        factor_of = factor_of * one(*cut)
    return factor_of


def scatter_about(stream_key, dims, deviation, reach, split=(), kind=jnp.bfloat16):
    array = deviation * jax.random.normal(stream_key, dims, jnp.float32)
    if split:
        array = array * block_scale(stream_key, dims, split, -0.22, 0.18)
    return jnp.clip(array, -reach, reach).astype(kind)


def setup_inputs(seed: int = 0) -> dict:
    splits = jax.random.split(jax.random.key(seed), 4)
    return {
        "eigvecs": scatter_about(splits[0], (N, M), 1.0, 6.0, ((0, 8), (1, 4)), jnp.float32),
        "reflectors": draw_reflectors(jax.random.fold_in(splits[3], 71), 0),
        "factors": draw_factors(jax.random.fold_in(splits[3], 71), 0),
    }


def reference(eigvecs, reflectors, factors):
    field = eigvecs
    for index in range(PANELS):
        vectors = reflectors[index]
        proj = lax.dot_general(vectors, field, (((0,), (0,)), ((), ())), precision=lax.Precision.HIGHEST, preferred_element_type=jnp.float32)
        coeffs = jnp.dot(factors[index], proj, precision=lax.Precision.HIGHEST, preferred_element_type=jnp.float32)
        field = field - jnp.dot(vectors, coeffs, precision=lax.Precision.HIGHEST, preferred_element_type=jnp.float32)
    return field
```

```python
import functools

import jax
import jax.numpy as jnp
from jax import lax
from jax.experimental import pallas as pl
from jax.experimental.pallas import tpu as pltpu
from jax.sharding import PartitionSpec as P


CORES = 2


def tile_of(rows):
    tile = 1024
    while rows % tile:
        tile //= 2
    return tile


def halves(value):
    high = value.astype(jnp.bfloat16)
    low = (value - high.astype(jnp.float32)).astype(jnp.bfloat16)
    return high, low


def three_pass(left, right, dims):
    left_high, left_low = halves(left)
    right_high, right_low = halves(right)
    dot = functools.partial(lax.dot_general, dimension_numbers=(dims, ((), ())), preferred_element_type=jnp.float32)
    return dot(left_high, right_high) + (dot(left_high, right_low) + dot(left_low, right_high))


def inner_kernel(first_ref, vectors_ref, field_ref, sums_ref):
    @pl.when(pl.program_id(0) == 0)
    def _():
        sums_ref[...] = jnp.zeros_like(sums_ref)

    sums_ref[...] += three_pass(vectors_ref[...], field_ref[...], ((0,), (0,)))


def inner(first, vectors, field):
    rows, width = vectors.shape
    columns = field.shape[1]
    tile = tile_of(rows)
    return pl.pallas_call(
        inner_kernel,
        out_shape=jax.ShapeDtypeStruct((width, columns), jnp.float32),
        grid_spec=pltpu.PrefetchScalarGridSpec(
            num_scalar_prefetch=1,
            grid=(rows // tile,),
            in_specs=[
                pl.BlockSpec((tile, width), lambda i, first: (i, 0)),
                pl.BlockSpec((tile, columns), lambda i, first: (first[0] * (rows // tile) + i, 0)),
            ],
            out_specs=pl.BlockSpec((width, columns), lambda i, first: (0, 0)),
        ),
        cost_estimate=pl.CostEstimate(flops=6 * rows * width * columns, bytes_accessed=4 * rows * (width + columns), transcendentals=0),
        name="inner",
    )(first, vectors, field)


def update_kernel(first_ref, vectors_ref, coeffs_ref, field_ref, *rest):
    rest[-1][...] = field_ref[...] - three_pass(vectors_ref[...], coeffs_ref[...], ((1,), (0,)))


def update(first, vectors, coeffs, field, target):
    rows, width = vectors.shape
    columns = field.shape[1]
    tile = tile_of(rows)
    steps = rows // tile
    in_specs = [
        pl.BlockSpec((tile, width), lambda i, first: (i, 0)),
        pl.BlockSpec((width, columns), lambda i, first: (0, 0)),
        pl.BlockSpec((tile, columns), lambda i, first: (first[0] * steps + i, 0)),
    ]
    operands = [first, vectors, coeffs, field]
    aliases = {}
    if target is not None:
        aliases = {len(operands): 0}
        operands.append(target)
        in_specs.append(pl.BlockSpec(memory_space=pl.ANY))
    return pl.pallas_call(
        update_kernel,
        out_shape=jax.ShapeDtypeStruct(field.shape, jnp.float32),
        grid_spec=pltpu.PrefetchScalarGridSpec(
            num_scalar_prefetch=1,
            grid=(steps,),
            in_specs=in_specs,
            out_specs=pl.BlockSpec((tile, columns), lambda i, first: (first[0] * steps + i, 0)),
        ),
        input_output_aliases=aliases,
        cost_estimate=pl.CostEstimate(flops=6 * rows * width * columns, bytes_accessed=4 * rows * (width + 2 * columns), transcendentals=0),
        name="update",
    )(*operands)


def take_kernel(panels_ref, out_ref):
    out_ref[...] = panels_ref[...]


def take(reflectors, index):
    _, rows, width = reflectors.shape
    tile = tile_of(rows)
    return pl.pallas_call(
        take_kernel,
        out_shape=jax.ShapeDtypeStruct((rows, width), jnp.float32),
        grid=(rows // tile,),
        in_specs=[pl.BlockSpec((None, tile, width), lambda i: (index, i, 0))],
        out_specs=pl.BlockSpec((tile, width), lambda i: (i, 0)),
        cost_estimate=pl.CostEstimate(flops=0, bytes_accessed=8 * rows * width, transcendentals=0),
        name="take",
    )(reflectors)


def after_kernel(value_ref, earlier_ref, out_ref):
    del value_ref, earlier_ref, out_ref


def after(value, earlier):
    return pl.pallas_call(
        after_kernel,
        out_shape=jax.ShapeDtypeStruct(value.shape, value.dtype),
        in_specs=[pl.BlockSpec(memory_space=pl.ANY)] * 2,
        out_specs=pl.BlockSpec(memory_space=pl.ANY),
        input_output_aliases={0: 0},
        cost_estimate=pl.CostEstimate(flops=0, bytes_accessed=1024, transcendentals=0),
        name="after",
    )(value, earlier)


def body(size, eigvecs, reflectors, factors):
    me = lax.axis_index("col")
    swap = [(j, j ^ 1) for j in range(size)]
    panels = factors.shape[0]
    shifts = range(CORES, size, CORES)

    def mate(vectors):
        return lax.ppermute(vectors, "col", swap)

    def send(own):
        return [lax.ppermute(own, "col", [(j, (j + shift) % size) for j in range(size)]) for shift in shifts]

    def place(owner):
        return jnp.reshape((owner + size) % size, (1,)).astype(jnp.int32)

    owns, fars = [], []
    for index in range(min(2, panels)):
        owns.append(take(reflectors, index))
        fars.append(send(owns[index]))

    field = eigvecs
    for index in range(panels):
        own = owns[index]
        parts = [(place(me), own), (place(me ^ 1), mate(own))]
        for shift, far in zip(shifts, fars[index]):
            if index:
                far = after(far, field)
            if index + 1 < panels:
                far = after(far, owns[index + 1])
            parts.append((place(me - shift), far))
        if index + 2 < panels:
            owns.append(after(take(reflectors, index + 2), parts[-1][1]))
            fars.append(send(owns[-1]))
        for shift, (_, far) in zip(shifts, parts[2:]):
            parts.append((place((me ^ 1) - shift), mate(far)))
        sums = None
        for first, vectors in parts:
            term = inner(first, vectors, field)
            sums = term if sums is None else sums + term
        sums = lax.psum(sums, "row")
        coeffs = jnp.dot(factors[index], sums, precision=lax.Precision.HIGHEST, preferred_element_type=jnp.float32)
        target = None
        for first, vectors in parts:
            target = update(first, vectors, coeffs, field, target)
        field = target
    return field


def solution(mesh):
    in_specs = (P("row", "col"), P(None, ("row", "col"), None), P())
    out_specs = P("row", "col")
    return jax.shard_map(functools.partial(body, mesh.shape["col"]), mesh=mesh, in_specs=in_specs, out_specs=out_specs, check_vma=False)
```
